128 devices in a mesh: row: 8 (over z_lo, y), col: 16 (over z_hi, x, core).
Axes of the slice: x: 4, y: 4, z: 4 (z_hi: 2, z_lo: 2; z = z_hi * 2 + z_lo), core: 2. Of those that a mesh axis runs over, the one named last changes fastest.
Arguments:
- initial_field: float32 [256, 256, 256], P(('row', 'col')), may hold values from -5 to 5
Outputs:
- advanced_field: float32 [256, 256, 256], P(('row', 'col'))
The draws below stay inside these ranges and needn't reach their ends.
All inputs are finite; a program needn't handle non-finite values.
Results may differ from the reference program's by a relative error of at most 0.0003.
Values sent between devices are 32-bit elements; how exact they have to be, the bound alone decides.
A program may use at most 64 MiB of HBM per device.

```python
import math
import jax
import jax.numpy as jnp

NX = 256
NY = 256
NZ = 256


def level_of(stream_key, dims, split, least, high):
    def one(position, blocks):
        heights = jax.random.uniform(jax.random.fold_in(jax.random.fold_in(stream_key, 6), position), (blocks,), jnp.float32, least / len(split), high / len(split))
        return jnp.repeat(jnp.exp(heights), dims[position] // blocks).reshape((-1,) + (1,) * (len(dims) - position - 1))

    gain = one(*split[0])
    for cut in split[1:]:
        gain = gain * one(*cut)
    return gain


def noise(own_key, dims, scale, bound, split=(), dtype=jnp.bfloat16):
    result = scale * jax.random.normal(own_key, dims, jnp.float32)
    if split:
        result = result * level_of(own_key, dims, split, -0.22, 0.18)
    return jnp.clip(result, -bound, bound).astype(dtype)


def setup_inputs(seed: int = 0) -> dict:
    key_of = jax.random.split(jax.random.key(seed), 2)
    initial_field = noise(key_of[0], (NX, NY, NZ), 1.0, 5.0, ((0, 128),), jnp.float32)
    return dict(initial_field=initial_field)


growth_rate = 0.3
quadratic = 1.0
time_step = 0.2
wave_scale = 4.0


def wavenumbers(count, offset, length):
    indices = (offset + jnp.arange(count)).astype(jnp.int32)
    signed = jnp.where(indices * 2 < length, indices, indices - length)
    return wave_scale * signed.astype(jnp.float32) / length


def phi_values(argument):
    within = jnp.abs(argument) < 1.0
    inside = jnp.where(within, argument, 0.0)
    outside = jnp.where(within, 2.0, argument)
    series = []
    for degree in (1, 2, 3):
        running = jnp.zeros_like(argument) + 1.0 / math.factorial(11 + degree)
        for exponent in range(10, -1, -1):
            running = running * inside + 1.0 / math.factorial(exponent + degree)
        series.append(running)
    growth_term = jnp.exp(outside)
    closed_one = (growth_term - 1.0) / outside
    closed_two = (growth_term - 1.0 - outside) / (outside * outside)
    closed_three = (growth_term - 1.0 - outside - 0.5 * outside * outside) / (outside * outside * outside)
    return (jnp.where(within, series[0], closed_one), jnp.where(within, series[1], closed_two), jnp.where(within, series[2], closed_three))


def step_factors(ksq):
    lin = growth_rate - (1.0 - ksq) * (1.0 - ksq)
    scaled = time_step * lin
    half_phi, _, _ = phi_values(0.5 * scaled)
    first_phi, second_phi, third_phi = phi_values(scaled)
    e_half = jnp.exp(0.5 * scaled)
    q_half = 0.5 * time_step * half_phi
    e_full = jnp.exp(scaled)
    f_one = time_step * (first_phi - 3.0 * second_phi + 4.0 * third_phi)
    f_two = time_step * (second_phi - 2.0 * third_phi)
    f_three = time_step * (4.0 * third_phi - second_phi)
    return e_half, q_half, e_full, f_one, f_two, f_three


def reaction(values):
    return quadratic * values * values - values * values * values


def reference(initial_field):
    wave_x = wavenumbers(NX, 0, NX)
    wave_y = wavenumbers(NY, 0, NY)
    wave_z = wavenumbers(NZ, 0, NZ)
    ksq = wave_x[:, None, None] ** 2 + wave_y[None, :, None] ** 2 + wave_z[None, None, :] ** 2
    e_half, q_half, e_full, f_one, f_two, f_three = step_factors(ksq)

    def forward_fft(values):
        return jnp.fft.fftn(values)

    def inverse_fft(spectrum):
        return jnp.fft.ifftn(spectrum).real

    state_hat = forward_fft(initial_field)
    react_u = forward_fft(reaction(initial_field))
    first_hat = e_half * state_hat + q_half * react_u
    react_a = forward_fft(reaction(inverse_fft(first_hat)))
    second_hat = e_half * state_hat + q_half * react_a
    react_b = forward_fft(reaction(inverse_fft(second_hat)))
    third_hat = e_half * first_hat + q_half * (2.0 * react_b - react_u)
    react_c = forward_fft(reaction(inverse_fft(third_hat)))
    new_hat = e_full * state_hat + f_one * react_u + 2.0 * f_two * (react_a + react_b) + f_three * react_c
    return inverse_fft(new_hat).astype(jnp.float32)
```

```python
import functools
import math

import jax
import jax.numpy as jnp
import numpy as np
from jax import lax
from jax.experimental import pallas as pl
from jax.experimental.pallas import tpu as pltpu
from jax.sharding import PartitionSpec as P

growth_rate = 0.3
quadratic = 1.0
time_step = 0.2
wave_scale = 4.0
MESH = pl.DeviceIdType.MESH
F32 = jnp.float32
BF16 = jnp.bfloat16


def basis(length):
    n = np.arange(length)
    half = length // 2
    mode = np.where(n <= half, n, n - half)
    angle = 2.0 * np.pi / length * ((mode[:, None] * n[None, :]) % length)
    table = np.where((n <= half)[:, None], np.cos(angle), np.sin(angle))
    scale = np.where((n == 0) | (n == half), 1.0 / length, 2.0 / length)
    return table * np.sqrt(scale)[:, None]


def split(value):
    high = value.astype(BF16)
    return high, (value - high.astype(F32)).astype(BF16)


def dot(left, right):
    return jnp.dot(left, right, preferred_element_type=F32)


def phi_values(argument):
    within = jnp.abs(argument) < 1.0
    inside = jnp.where(within, argument, 0.0)
    outside = jnp.where(within, 2.0, argument)
    series = []
    for degree in (1, 2, 3):
        running = jnp.zeros_like(argument) + 1.0 / math.factorial(11 + degree)
        for exponent in range(10, -1, -1):
            running = running * inside + 1.0 / math.factorial(exponent + degree)
        series.append(running)
    growth_term = jnp.exp(outside)
    closed_one = (growth_term - 1.0) / outside
    closed_two = (growth_term - 1.0 - outside) / (outside * outside)
    closed_three = (growth_term - 1.0 - outside - 0.5 * outside * outside) / (
        outside * outside * outside
    )
    return (
        jnp.where(within, series[0], closed_one),
        jnp.where(within, series[1], closed_two),
        jnp.where(within, series[2], closed_three),
    )


def step_factors(ksq):
    lin = growth_rate - (1.0 - ksq) * (1.0 - ksq)
    scaled = time_step * lin
    half_phi, _, _ = phi_values(0.5 * scaled)
    first_phi, second_phi, third_phi = phi_values(scaled)
    e_half = jnp.exp(0.5 * scaled)
    q_half = 0.5 * time_step * half_phi
    e_full = jnp.exp(scaled)
    f_one = time_step * (first_phi - 3.0 * second_phi + 4.0 * third_phi)
    f_two = time_step * (second_phi - 2.0 * third_phi)
    f_three = time_step * (4.0 * third_phi - second_phi)
    return (e_half, q_half, e_full, f_one, f_two, f_three)


def reaction(values):
    return quadratic * values * values - values * values * values


def wave(index, size):
    mode = jnp.where(index * 2 <= size, index, index - size // 2)
    return wave_scale * mode.astype(F32) / size


def kernel(
    sizes, offsets, field, qh_ref, ql_ref, th_ref, tl_ref, out_ref,
    send_f, recv_f, send_i, recv_i, held, factors,
    fsend, frecv, isend, irecv,
):
    rows, cols, size_x, size_y, size_z = sizes
    devices = rows * cols
    row = lax.axis_index("row")
    col = lax.axis_index("col")
    me = row * cols + col
    groups = size_y // 8
    count = devices - 1

    def peer(step):
        dr, dc = offsets(step, row, col)
        return dr, dc

    barrier = pltpu.get_barrier_semaphore()

    def greet(step, carry):
        pl.semaphore_signal(barrier, inc=1, device_id=peer(step), device_id_type=MESH)
        return carry

    lax.fori_loop(0, count, greet, 0)

    def tile(index):
        return pl.ds(pl.multiple_of(index * 8, 8), 8)

    def send(source, target, ssem, rsem):
        def one(step, carry):
            pr, pc = peer(step)
            pltpu.make_async_remote_copy(
                src_ref=source.at[tile(pr * cols + pc), :],
                dst_ref=target.at[tile(me), :],
                send_sem=ssem, recv_sem=rsem,
                device_id=(pr, pc), device_id_type=MESH,
            ).start()
            return carry

        lax.fori_loop(0, count, one, 0)
        target[tile(me), :] = source[tile(me), :]

    def drain(ref, sem):
        part = ref.at[pl.ds(0, count * 8), :]
        pltpu.make_async_copy(part, part, sem).wait()

    low = lax.broadcasted_iota(jnp.int32, (groups, 8, 128), 1) < 4

    def to_blocks(values, target):
        vh, vl = split(values)
        along_z = dot(vh, th_ref[...]) + dot(vl, th_ref[...]) + dot(vh, tl_ref[...])
        both = []
        for plane in range(2):
            wh, wl = split(along_z[plane * size_y : (plane + 1) * size_y])
            both.append(dot(qh_ref[...], wh) + dot(qh_ref[...], wl) + dot(ql_ref[...], wh))
        for part in range(2):
            a = both[0][:, part * 128 : part * 128 + 128].reshape(groups, 8, 128)
            b = both[1][:, part * 128 : part * 128 + 128].reshape(groups, 8, 128)
            first = jnp.where(low, a, pltpu.roll(b, 4, 1))
            second = jnp.where(low, pltpu.roll(a, 4, 1), b)
            base = part * 2 * size_y
            target[base : base + size_y, :] = first.reshape(size_y, 128)
            target[base + size_y : base + 2 * size_y, :] = second.reshape(size_y, 128)

    def from_blocks(source):
        planes = ([], [])
        for part in range(2):
            base = part * 2 * size_y
            first = source[base : base + size_y, :].reshape(groups, 8, 128)
            second = source[base + size_y : base + 2 * size_y, :].reshape(groups, 8, 128)
            a = jnp.where(low, first, pltpu.roll(second, 4, 1))
            b = jnp.where(low, pltpu.roll(first, 4, 1), second)
            planes[0].append(a.reshape(size_y, 128))
            planes[1].append(b.reshape(size_y, 128))
        done = []
        for plane in range(2):
            wh, wl = split(jnp.concatenate(planes[plane], axis=1))
            along_y = dot(th_ref[...], wh) + dot(th_ref[...], wl) + dot(tl_ref[...], wh)
            vh, vl = split(along_y)
            done.append(dot(vh, qh_ref[...]) + dot(vl, qh_ref[...]) + dot(vh, ql_ref[...]))
        return jnp.concatenate(done, axis=0)

    def gathered(source, pair):
        parts = [source[pl.ds(2 * pair + k, size_x, stride=4), :] for k in range(2)]
        gh, gl = split(jnp.concatenate(parts, axis=1))
        return dot(qh_ref[...], gh) + dot(qh_ref[...], gl) + dot(ql_ref[...], gh)

    def scattered(values, pair):
        vh, vl = split(values)
        along_x = dot(th_ref[...], vh) + dot(th_ref[...], vl) + dot(tl_ref[...], vh)
        for k in range(2):
            send_i[pl.ds(2 * pair + k, size_x, stride=4), :] = along_x[:, k * 128 : k * 128 + 128]

    values = field[...]
    to_blocks(values, send_f.at[0])
    pl.semaphore_wait(barrier, count)
    send(send_f.at[0], recv_f.at[0], fsend.at[0], frecv.at[0])
    to_blocks(reaction(values), send_f.at[1])
    send(send_f.at[1], recv_f.at[1], fsend.at[1], frecv.at[1])

    part = me // (devices // 2)
    half = (me // (devices // 4)) % 2
    group = me % (devices // 4)
    lane = lax.broadcasted_iota(jnp.int32, (8, 512), 1)
    ky = wave(group * 8 + half * 4 + lane // 128, size_y)
    kz = wave(part * 128 + lane % 128, size_z)
    kyz = ky * ky + kz * kz

    def factor_rows(block, carry):
        at = pl.ds(pl.multiple_of(block * 8, 8), 8)
        kx = wave(block * 8 + lax.broadcasted_iota(jnp.int32, (8, 512), 0), size_x)
        for index, value in enumerate(step_factors(kx * kx + kyz)):
            factors[index, at, :] = value
        return carry

    lax.fori_loop(0, size_x // 8, factor_rows, 0)

    E_HALF, Q_HALF, E_FULL, F_ONE, F_TWO, F_THREE = range(6)
    for pair in range(2):
        lanes = slice(pair * 256, pair * 256 + 256)
        if pair == 0:
            drain(recv_f.at[0], frecv.at[0])
            drain(recv_f.at[1], frecv.at[1])
        state = gathered(recv_f.at[0], pair)
        react_u = gathered(recv_f.at[1], pair)
        moved = factors[E_HALF, :, lanes] * state
        pushed = factors[Q_HALF, :, lanes] * react_u
        first = moved + pushed
        scattered(first, pair)
        held[0, :, lanes] = moved
        held[1, :, lanes] = factors[E_HALF, :, lanes] * first - pushed
        held[2, :, lanes] = factors[E_FULL, :, lanes] * state + factors[F_ONE, :, lanes] * react_u
    send(send_i, recv_i, isend, irecv)
    drain(send_f.at[0], fsend.at[0])
    drain(send_f.at[1], fsend.at[1])

    for stage in range(4):
        drain(recv_i, irecv)
        drain(send_i, isend)
        values = from_blocks(recv_i)
        if stage == 3:
            out_ref[...] = values
            break
        to_blocks(reaction(values), send_f.at[0])
        send(send_f.at[0], recv_f.at[0], fsend.at[0], frecv.at[0])
        drain(recv_f.at[0], frecv.at[0])
        drain(send_f.at[0], fsend.at[0])
        for pair in range(2):
            lanes = slice(pair * 256, pair * 256 + 256)
            react = gathered(recv_f.at[0], pair)
            if stage == 0:
                scattered(held[0, :, lanes] + factors[Q_HALF, :, lanes] * react, pair)
                held[2, :, lanes] += 2.0 * factors[F_TWO, :, lanes] * react
            if stage == 1:
                scattered(held[1, :, lanes] + 2.0 * (factors[Q_HALF, :, lanes] * react), pair)
                held[2, :, lanes] += 2.0 * factors[F_TWO, :, lanes] * react
            if stage == 2:
                scattered(held[2, :, lanes] + factors[F_THREE, :, lanes] * react, pair)
        send(send_i, recv_i, isend, irecv)


def schedule(step, row, col):
    def hop(code):
        return (2 + code + code // 2 + 2 * (code // 3)) % 4

    dz = hop(step // 32)
    dy = hop((step // 8) % 4)
    dx = hop((step // 2) % 4)
    dc = 1 - step % 2
    z = (col // 8) * 2 + row // 4
    y = row % 4
    x = (col // 2) % 4
    core = col % 2
    z = (z + dz) % 4
    y = (y + dy) % 4
    x = (x + dx) % 4
    core = (core + dc) % 2
    return (z % 2) * 4 + y, (z // 2) * 8 + x * 2 + core


def solution(mesh):
    rows, cols = mesh.shape["row"], mesh.shape["col"]
    table = basis(256).astype(np.float32)

    def halves(values):
        high = values.astype(BF16)
        return high, (values - high.astype(np.float32)).astype(BF16)

    qh, ql = halves(table)
    th, tl = halves(np.ascontiguousarray(table.T))

    def body(field):
        planes, size_y, size_z = field.shape
        size_x = planes * rows * cols
        sizes = (rows, cols, size_x, size_y, size_z)
        flat = field.reshape(planes * size_y, size_z)
        vmem = pl.BlockSpec(memory_space=pltpu.VMEM)
        out = pl.pallas_call(
            functools.partial(kernel, sizes, schedule),
            out_shape=jax.ShapeDtypeStruct(flat.shape, F32),
            in_specs=[vmem] * 5,
            out_specs=vmem,
            scratch_shapes=[
                pltpu.VMEM((2, size_x * 4, 128), F32),
                pltpu.VMEM((2, size_x * 4, 128), F32),
                pltpu.VMEM((size_x * 4, 128), F32),
                pltpu.VMEM((size_x * 4, 128), F32),
                pltpu.VMEM((3, size_x, 512), F32),
                pltpu.VMEM((6, size_x, 512), F32),
                pltpu.SemaphoreType.DMA((2,)),
                pltpu.SemaphoreType.DMA((2,)),
                pltpu.SemaphoreType.DMA,
                pltpu.SemaphoreType.DMA,
            ],
            compiler_params=pltpu.CompilerParams(
                collective_id=0, has_side_effects=True, vmem_limit_bytes=48 * 1024 * 1024
            ),
        )(flat, jnp.asarray(qh), jnp.asarray(ql), jnp.asarray(th), jnp.asarray(tl))
        return out.reshape(field.shape)

    placed = (P(("row", "col"), None, None),)
    return jax.shard_map(
        body, mesh=mesh, in_specs=placed, out_specs=P(("row", "col"), None, None), check_vma=False
    )
```

```python
import functools
import math

import jax
import jax.numpy as jnp
import numpy as np
from jax import lax
from jax.experimental import pallas as pl
from jax.experimental.pallas import tpu as pltpu
from jax.sharding import PartitionSpec as P

growth_rate = 0.3
quadratic = 1.0
time_step = 0.2
wave_scale = 4.0
LOGICAL = pl.DeviceIdType.LOGICAL
F32 = jnp.float32
BF16 = jnp.bfloat16


def basis(length):
    n = np.arange(length)
    half = length // 2
    mode = np.where(n <= half, n, n - half)
    angle = 2.0 * np.pi / length * ((mode[:, None] * n[None, :]) % length)
    table = np.where((n <= half)[:, None], np.cos(angle), np.sin(angle))
    scale = np.where((n == 0) | (n == half), 1.0 / length, 2.0 / length)
    return table * np.sqrt(scale)[:, None]


def split(value):
    high = value.astype(BF16)
    return high, (value - high.astype(F32)).astype(BF16)


def dot(left, right):
    return jnp.dot(left, right, preferred_element_type=F32)


def phi_values(argument):
    within = jnp.abs(argument) < 1.0
    inside = jnp.where(within, argument, 0.0)
    outside = jnp.where(within, 2.0, argument)
    series = []
    for degree in (1, 2, 3):
        running = jnp.zeros_like(argument) + 1.0 / math.factorial(11 + degree)
        for exponent in range(10, -1, -1):
            running = running * inside + 1.0 / math.factorial(exponent + degree)
        series.append(running)
    growth_term = jnp.exp(outside)
    closed_one = (growth_term - 1.0) / outside
    closed_two = (growth_term - 1.0 - outside) / (outside * outside)
    closed_three = (growth_term - 1.0 - outside - 0.5 * outside * outside) / (
        outside * outside * outside
    )
    return (
        jnp.where(within, series[0], closed_one),
        jnp.where(within, series[1], closed_two),
        jnp.where(within, series[2], closed_three),
    )


def step_factors(ksq):
    lin = growth_rate - (1.0 - ksq) * (1.0 - ksq)
    scaled = time_step * lin
    half_phi, _, _ = phi_values(0.5 * scaled)
    first_phi, second_phi, third_phi = phi_values(scaled)
    e_half = jnp.exp(0.5 * scaled)
    q_half = 0.5 * time_step * half_phi
    e_full = jnp.exp(scaled)
    f_one = time_step * (first_phi - 3.0 * second_phi + 4.0 * third_phi)
    f_two = time_step * (second_phi - 2.0 * third_phi)
    f_three = time_step * (4.0 * third_phi - second_phi)
    return (e_half, q_half, e_full, f_one, f_two, f_three)


def reaction(values):
    return quadratic * values * values - values * values * values


def wave(index, size):
    mode = jnp.where(index * 2 <= size, index, index - size // 2)
    return wave_scale * mode.astype(F32) / size


def kernel(
    sizes, offsets, field, qh_ref, ql_ref, th_ref, tl_ref, out_ref,
    send_p, recv_p, send_f, recv_f, send_i, recv_i, held, factors,
    psend, precv, fsend, frecv, isend, irecv,
):
    rows, cols, size_x, size_y, size_z = sizes
    devices = rows * cols
    row = lax.axis_index("row")
    col = lax.axis_index("col")
    me = row * cols + col
    groups = size_y // 8
    count = devices - 1

    z, y = (col // 8) * 2 + row // 4, row % 4
    x, core = (col // 2) % 4, col % 2
    along_zy = {}
    along_xc = {}
    for far in range(4):
        other = (z + far) % 4
        base = (other % 2) * (4 * cols) + (other // 2) * 8
        for near in range(4):
            along_zy[far, near] = base + ((y + near) % 4) * cols
        for near in range(2):
            along_xc[far, near] = ((x + far) % 4) * 2 + (core + near) % 2
    peers = [along_zy[o[0], o[1]] + along_xc[o[2], o[3]] for o in offsets]

    barrier = pltpu.get_barrier_semaphore()
    for other in peers:
        pl.semaphore_signal(barrier, inc=1, device_id=other, device_id_type=LOGICAL)

    def tile(index):
        return pl.ds(pl.multiple_of(index * 8, 8), 8)

    def send(source, target, ssem, rsem):
        for other in peers:
            pltpu.make_async_remote_copy(
                src_ref=source.at[..., tile(other), :],
                dst_ref=target.at[..., tile(me), :],
                send_sem=ssem, recv_sem=rsem,
                device_id=other, device_id_type=LOGICAL,
            ).start()
        target[..., tile(me), :] = source[..., tile(me), :]

    def drain(ref, sem):
        part = ref.at[..., pl.ds(0, count * 8), :]
        pltpu.make_async_copy(part, part, sem).wait()

    low = lax.broadcasted_iota(jnp.int32, (groups, 8, 128), 1) < 4

    def to_blocks(values, target):
        vh, vl = split(values)
        along_z = dot(vh, th_ref[...]) + dot(vl, th_ref[...]) + dot(vh, tl_ref[...])
        both = []
        for plane in range(2):
            wh, wl = split(along_z[plane * size_y : (plane + 1) * size_y])
            both.append(dot(qh_ref[...], wh) + dot(qh_ref[...], wl) + dot(ql_ref[...], wh))
        for part in range(2):
            a = both[0][:, part * 128 : part * 128 + 128].reshape(groups, 8, 128)
            b = both[1][:, part * 128 : part * 128 + 128].reshape(groups, 8, 128)
            first = jnp.where(low, a, pltpu.roll(b, 4, 1))
            second = jnp.where(low, pltpu.roll(a, 4, 1), b)
            base = part * 2 * size_y
            target[base : base + size_y, :] = first.reshape(size_y, 128)
            target[base + size_y : base + 2 * size_y, :] = second.reshape(size_y, 128)

    def from_blocks(source):
        planes = ([], [])
        for part in range(2):
            base = part * 2 * size_y
            first = source[base : base + size_y, :].reshape(groups, 8, 128)
            second = source[base + size_y : base + 2 * size_y, :].reshape(groups, 8, 128)
            a = jnp.where(low, first, pltpu.roll(second, 4, 1))
            b = jnp.where(low, pltpu.roll(first, 4, 1), second)
            planes[0].append(a.reshape(size_y, 128))
            planes[1].append(b.reshape(size_y, 128))
        done = []
        for plane in range(2):
            wh, wl = split(jnp.concatenate(planes[plane], axis=1))
            along_y = dot(th_ref[...], wh) + dot(th_ref[...], wl) + dot(tl_ref[...], wh)
            vh, vl = split(along_y)
            done.append(dot(vh, qh_ref[...]) + dot(vl, qh_ref[...]) + dot(vh, ql_ref[...]))
        return jnp.concatenate(done, axis=0)

    def gathered(source, pair):
        parts = [source[pl.ds(2 * pair + k, size_x, stride=4), :] for k in range(2)]
        gh, gl = split(jnp.concatenate(parts, axis=1))
        return dot(qh_ref[...], gh) + dot(qh_ref[...], gl) + dot(ql_ref[...], gh)

    def scattered(values, pair):
        vh, vl = split(values)
        along_x = dot(th_ref[...], vh) + dot(th_ref[...], vl) + dot(tl_ref[...], vh)
        for k in range(2):
            send_i[pl.ds(2 * pair + k, size_x, stride=4), :] = along_x[:, k * 128 : k * 128 + 128]

    values = field[...]
    to_blocks(values, send_p.at[0])
    to_blocks(reaction(values), send_p.at[1])
    pl.semaphore_wait(barrier, count)
    send(send_p, recv_p, psend, precv)

    part = me // (devices // 2)
    half = (me // (devices // 4)) % 2
    group = me % (devices // 4)
    lane = lax.broadcasted_iota(jnp.int32, (8, 512), 1)
    ky = wave(group * 8 + half * 4 + lane // 128, size_y)
    kz = wave(part * 128 + lane % 128, size_z)
    kyz = ky * ky + kz * kz

    def factor_rows(block, carry):
        at = pl.ds(pl.multiple_of(block * 8, 8), 8)
        kx = wave(block * 8 + lax.broadcasted_iota(jnp.int32, (8, 512), 0), size_x)
        for index, value in enumerate(step_factors(kx * kx + kyz)):
            factors[index, at, :] = value
        return carry

    lax.fori_loop(0, size_x // 8, factor_rows, 0)

    E_HALF, Q_HALF, E_FULL, F_ONE, F_TWO, F_THREE = range(6)
    for pair in range(2):
        lanes = slice(pair * 256, pair * 256 + 256)
        if pair == 0:
            drain(recv_p, precv)
        state = gathered(recv_p.at[0], pair)
        react_u = gathered(recv_p.at[1], pair)
        moved = factors[E_HALF, :, lanes] * state
        pushed = factors[Q_HALF, :, lanes] * react_u
        first = moved + pushed
        scattered(first, pair)
        held[0, :, lanes] = moved
        held[1, :, lanes] = factors[E_HALF, :, lanes] * first - pushed
        held[2, :, lanes] = factors[E_FULL, :, lanes] * state + factors[F_ONE, :, lanes] * react_u
    send(send_i, recv_i, isend, irecv)
    drain(send_p, psend)

    for stage in range(4):
        drain(recv_i, irecv)
        drain(send_i, isend)
        values = from_blocks(recv_i)
        if stage == 3:
            out_ref[...] = values
            break
        to_blocks(reaction(values), send_f)
        send(send_f, recv_f, fsend, frecv)
        drain(recv_f, frecv)
        drain(send_f, fsend)
        for pair in range(2):
            lanes = slice(pair * 256, pair * 256 + 256)
            react = gathered(recv_f, pair)
            if stage == 0:
                scattered(held[0, :, lanes] + factors[Q_HALF, :, lanes] * react, pair)
                held[2, :, lanes] += 2.0 * factors[F_TWO, :, lanes] * react
            if stage == 1:
                scattered(held[1, :, lanes] + 2.0 * (factors[Q_HALF, :, lanes] * react), pair)
                held[2, :, lanes] += 2.0 * factors[F_TWO, :, lanes] * react
            if stage == 2:
                scattered(held[2, :, lanes] + factors[F_THREE, :, lanes] * react, pair)
        send(send_i, recv_i, isend, irecv)


def hops(offset):
    return sum(min(o, 4 - o) for o in offset[:3])


def schedule():
    every = [(a, b, c, d) for a in range(4) for b in range(4) for c in range(4) for d in range(2)]
    return sorted(every[1:], key=lambda offset: -2 * hops(offset) - offset[3])


def solution(mesh):
    rows, cols = mesh.shape["row"], mesh.shape["col"]
    table = basis(256).astype(np.float32)

    def halves(values):
        high = values.astype(BF16)
        return high, (values - high.astype(np.float32)).astype(BF16)

    qh, ql = halves(table)
    th, tl = halves(np.ascontiguousarray(table.T))

    def body(field):
        planes, size_y, size_z = field.shape
        size_x = planes * rows * cols
        sizes = (rows, cols, size_x, size_y, size_z)
        flat = field.reshape(planes * size_y, size_z)
        vmem = pl.BlockSpec(memory_space=pltpu.VMEM)
        out = pl.pallas_call(
            functools.partial(kernel, sizes, schedule()),
            out_shape=jax.ShapeDtypeStruct(flat.shape, F32),
            in_specs=[vmem] * 5,
            out_specs=vmem,
            scratch_shapes=[
                pltpu.VMEM((2, size_x * 4, 128), F32),
                pltpu.VMEM((2, size_x * 4, 128), F32),
                *[pltpu.VMEM((size_x * 4, 128), F32)] * 4,
                pltpu.VMEM((3, size_x, 512), F32),
                pltpu.VMEM((6, size_x, 512), F32),
                *[pltpu.SemaphoreType.DMA] * 6,
            ],
            compiler_params=pltpu.CompilerParams(
                collective_id=0, has_side_effects=True, vmem_limit_bytes=48 * 1024 * 1024
            ),
        )(flat, jnp.asarray(qh), jnp.asarray(ql), jnp.asarray(th), jnp.asarray(tl))
        return out.reshape(field.shape)

    placed = (P(("row", "col"), None, None),)
    return jax.shard_map(
        body, mesh=mesh, in_specs=placed, out_specs=P(("row", "col"), None, None), check_vma=False
    )
```

```python
import functools
import math

import jax
import jax.numpy as jnp
import numpy as np
from jax import lax
from jax.experimental import pallas as pl
from jax.experimental.pallas import tpu as pltpu
from jax.sharding import PartitionSpec as P

growth_rate = 0.3
quadratic = 1.0
time_step = 0.2
wave_scale = 4.0
LOGICAL = pl.DeviceIdType.LOGICAL
F32 = jnp.float32
BF16 = jnp.bfloat16


def basis(length):
    n = np.arange(length)
    half = length // 2
    mode = np.where(n <= half, n, n - half)
    angle = 2.0 * np.pi / length * ((mode[:, None] * n[None, :]) % length)
    table = np.where((n <= half)[:, None], np.cos(angle), np.sin(angle))
    scale = np.where((n == 0) | (n == half), 1.0 / length, 2.0 / length)
    return table * np.sqrt(scale)[:, None]


def split(value):
    high = value.astype(BF16)
    return high, (value - high.astype(F32)).astype(BF16)


def dot(left, right):
    return jnp.dot(left, right, preferred_element_type=F32)


def phi_values(argument):
    within = jnp.abs(argument) < 1.0
    inside = jnp.where(within, argument, 0.0)
    outside = jnp.where(within, 2.0, argument)
    series = []
    for degree in (1, 2, 3):
        running = jnp.zeros_like(argument) + 1.0 / math.factorial(11 + degree)
        for exponent in range(10, -1, -1):
            running = running * inside + 1.0 / math.factorial(exponent + degree)
        series.append(running)
    growth_term = jnp.exp(outside)
    closed_one = (growth_term - 1.0) / outside
    closed_two = (growth_term - 1.0 - outside) / (outside * outside)
    closed_three = (growth_term - 1.0 - outside - 0.5 * outside * outside) / (
        outside * outside * outside
    )
    return (
        jnp.where(within, series[0], closed_one),
        jnp.where(within, series[1], closed_two),
        jnp.where(within, series[2], closed_three),
    )


def step_factors(ksq):
    lin = growth_rate - (1.0 - ksq) * (1.0 - ksq)
    scaled = time_step * lin
    half_phi, _, _ = phi_values(0.5 * scaled)
    first_phi, second_phi, third_phi = phi_values(scaled)
    e_half = jnp.exp(0.5 * scaled)
    q_half = 0.5 * time_step * half_phi
    e_full = jnp.exp(scaled)
    f_one = time_step * (first_phi - 3.0 * second_phi + 4.0 * third_phi)
    f_two = time_step * (second_phi - 2.0 * third_phi)
    f_three = time_step * (4.0 * third_phi - second_phi)
    return (e_half, q_half, e_full, f_one, f_two, f_three)


def reaction(values):
    return quadratic * values * values - values * values * values


def wave(index, size):
    mode = jnp.where(index * 2 <= size, index, index - size // 2)
    return wave_scale * mode.astype(F32) / size


def kernel(
    sizes, offsets, field_hbm, qh_hbm, ql_hbm, th_hbm, tl_hbm, out_ref,
    field, qh_ref, ql_ref, th_ref, tl_ref,
    send_p, recv_p, send_f, recv_f, send_i, recv_i, held, factors,
    loaded, psend, precv, fsend, frecv, isend, irecv,
):
    rows, cols, size_x, size_y, size_z = sizes
    devices = rows * cols
    row = lax.axis_index("row")
    col = lax.axis_index("col")
    me = row * cols + col
    quarter = size_y // 4
    count = devices - 1

    z, y = (col // 8) * 2 + row // 4, row % 4
    x, core = (col // 2) % 4, col % 2
    along_zy = {}
    along_xc = {}
    for far in range(4):
        other = (z + far) % 4
        base = (other % 2) * (4 * cols) + (other // 2) * 8
        for near in range(4):
            along_zy[far, near] = base + ((y + near) % 4) * cols
        for near in range(2):
            along_xc[far, near] = ((x + far) % 4) * 2 + (core + near) % 2
    peers = [along_zy[o[0], o[1]] + along_xc[o[2], o[3]] for o in offsets]

    barrier = pltpu.get_barrier_semaphore()
    for other in peers:
        pl.semaphore_signal(barrier, inc=1, device_id=other, device_id_type=LOGICAL)

    loads = [
        pltpu.make_async_copy(source, target, loaded.at[index])
        for index, (source, target) in enumerate(
            ((field_hbm, field), (th_hbm, th_ref), (tl_hbm, tl_ref), (qh_hbm, qh_ref), (ql_hbm, ql_ref))
        )
    ]
    for load in loads:
        load.start()

    def tile(index):
        return pl.ds(pl.multiple_of(index * 4, 4), 4)

    def send(source, target, ssem, rsem):
        for other in peers:
            pltpu.make_async_remote_copy(
                src_ref=source.at[..., tile(other), :],
                dst_ref=target.at[..., tile(me), :],
                send_sem=ssem, recv_sem=rsem,
                device_id=other, device_id_type=LOGICAL,
            ).start()
        target[..., tile(me), :] = source[..., tile(me), :]

    def drain(ref, sem):
        part = ref.at[..., pl.ds(0, count * 4), :]
        pltpu.make_async_copy(part, part, sem).wait()

    def along_zf(values):
        vh, vl = split(values)
        moved = dot(vh, th_ref[...]) + dot(vl, th_ref[...]) + dot(vh, tl_ref[...])
        return split(jnp.concatenate([moved[:size_y], moved[size_y:]], axis=1))

    def along_yf(halves, chunk, target):
        wh, wl = halves
        at = slice(chunk * 2 * quarter, (chunk + 1) * 2 * quarter)
        moved = dot(qh_ref[at, :], wh) + dot(qh_ref[at, :], wl) + dot(ql_ref[at, :], wh)
        for plane in range(2):
            for part in range(2):
                lanes = slice(plane * size_z + part * 128, plane * size_z + part * 128 + 128)
                for k in range(2):
                    start = part * 4 * quarter + plane * 2 + k
                    target[pl.ds(start, quarter, stride=4), :] = moved[
                        k * quarter : (k + 1) * quarter, lanes
                    ]

    def along_yi(source, chunk):
        lines = []
        for k in range(2):
            across = []
            for plane in range(2):
                for part in range(2):
                    start = part * 4 * quarter + plane * 2 + k
                    across.append(source[pl.ds(start, quarter, stride=4), :])
            lines.append(jnp.concatenate(across, axis=1))
        wh, wl = split(jnp.concatenate(lines, axis=0))
        at = slice(chunk * 2 * quarter, (chunk + 1) * 2 * quarter)
        return dot(th_ref[:, at], wh) + dot(th_ref[:, at], wl) + dot(tl_ref[:, at], wh)

    def along_zi(moved):
        vh, vl = split(jnp.concatenate([moved[:, :size_z], moved[:, size_z:]], axis=0))
        return dot(vh, qh_ref[...]) + dot(vl, qh_ref[...]) + dot(vh, ql_ref[...])

    def gathered(source):
        parts = [source[pl.ds(k, size_x, stride=2), :] for k in range(2)]
        gh, gl = split(jnp.concatenate(parts, axis=1))
        return dot(qh_ref[...], gh) + dot(qh_ref[...], gl) + dot(ql_ref[...], gh)

    def scattered(values, target):
        vh, vl = split(values)
        moved = dot(th_ref[...], vh) + dot(th_ref[...], vl) + dot(tl_ref[...], vh)
        for k in range(2):
            target[pl.ds(k, size_x, stride=2), :] = moved[:, k * 128 : k * 128 + 128]

    for load in loads:
        load.wait()
    values = field[...]
    straight = along_zf(values)
    reacted = along_zf(reaction(values))
    for chunk in range(2):
        along_yf(straight, chunk, send_p.at[chunk, 0])
        along_yf(reacted, chunk, send_p.at[chunk, 1])
        if chunk == 0:
            pl.semaphore_wait(barrier, count)
        send(send_p.at[chunk], recv_p.at[chunk], psend.at[chunk], precv.at[chunk])

    part = me // (devices // 2)
    group = me % (devices // 2)
    lane = lax.broadcasted_iota(jnp.int32, (8, 512), 1)
    ky = wave((lane // 128) * quarter + group, size_y)
    kz = wave(part * 128 + lane % 128, size_z)
    kyz = ky * ky + kz * kz

    def factor_rows(block, carry):
        at = pl.ds(pl.multiple_of(block * 8, 8), 8)
        kx = wave(block * 8 + lax.broadcasted_iota(jnp.int32, (8, 512), 0), size_x)
        for index, value in enumerate(step_factors(kx * kx + kyz)):
            factors[index, at, :] = value
        return carry

    lax.fori_loop(0, size_x // 8, factor_rows, 0)

    E_HALF, Q_HALF, E_FULL, F_ONE, F_TWO, F_THREE = range(6)
    for chunk in range(2):
        lanes = slice(chunk * 256, chunk * 256 + 256)
        drain(recv_p.at[chunk], precv.at[chunk])
        state = gathered(recv_p.at[chunk, 0])
        react_u = gathered(recv_p.at[chunk, 1])
        moved = factors[E_HALF, :, lanes] * state
        pushed = factors[Q_HALF, :, lanes] * react_u
        first = moved + pushed
        scattered(first, send_i.at[chunk])
        send(send_i.at[chunk], recv_i.at[chunk], isend.at[chunk], irecv.at[chunk])
        held[0, :, lanes] = moved
        held[1, :, lanes] = factors[E_HALF, :, lanes] * first - pushed
        held[2, :, lanes] = factors[E_FULL, :, lanes] * state + factors[F_ONE, :, lanes] * react_u
    for chunk in range(2):
        drain(send_p.at[chunk], psend.at[chunk])

    for stage in range(4):
        drain(recv_i.at[0], irecv.at[0])
        moved = along_yi(recv_i.at[0], 0)
        drain(recv_i.at[1], irecv.at[1])
        values = along_zi(moved + along_yi(recv_i.at[1], 1))
        for chunk in range(2):
            drain(send_i.at[chunk], isend.at[chunk])
        if stage == 3:
            out_ref[...] = values
            break
        halves = along_zf(reaction(values))
        for chunk in range(2):
            along_yf(halves, chunk, send_f.at[chunk])
            send(send_f.at[chunk], recv_f.at[chunk], fsend.at[chunk], frecv.at[chunk])
        for chunk in range(2):
            lanes = slice(chunk * 256, chunk * 256 + 256)
            drain(recv_f.at[chunk], frecv.at[chunk])
            react = gathered(recv_f.at[chunk])
            if stage == 0:
                spectrum = held[0, :, lanes] + factors[Q_HALF, :, lanes] * react
            if stage == 1:
                spectrum = held[1, :, lanes] + 2.0 * (factors[Q_HALF, :, lanes] * react)
            if stage == 2:
                spectrum = held[2, :, lanes] + factors[F_THREE, :, lanes] * react
            scattered(spectrum, send_i.at[chunk])
            send(send_i.at[chunk], recv_i.at[chunk], isend.at[chunk], irecv.at[chunk])
            if stage < 2:
                held[2, :, lanes] += 2.0 * factors[F_TWO, :, lanes] * react
        for chunk in range(2):
            drain(send_f.at[chunk], fsend.at[chunk])


def hops(offset):
    return sum(min(o, 4 - o) for o in offset[:3])


def schedule():
    every = [(a, b, c, d) for a in range(4) for b in range(4) for c in range(4) for d in range(2)]
    return sorted(every[1:], key=lambda offset: -2 * hops(offset) - offset[3])


def solution(mesh):
    rows, cols = mesh.shape["row"], mesh.shape["col"]
    table = basis(256).astype(np.float32)

    def halves(values):
        high = values.astype(BF16)
        return high, (values - high.astype(np.float32)).astype(BF16)

    qh, ql = halves(table)
    th, tl = halves(np.ascontiguousarray(table.T))

    def body(field):
        planes, size_y, size_z = field.shape
        size_x = planes * rows * cols
        sizes = (rows, cols, size_x, size_y, size_z)
        flat = field.reshape(planes * size_y, size_z)
        hbm = pl.BlockSpec(memory_space=pltpu.HBM)
        tables = [pltpu.VMEM(table.shape, BF16)] * 4
        out = pl.pallas_call(
            functools.partial(kernel, sizes, schedule()),
            out_shape=jax.ShapeDtypeStruct(flat.shape, F32),
            in_specs=[hbm] * 5,
            out_specs=pl.BlockSpec(memory_space=pltpu.VMEM),
            scratch_shapes=[
                pltpu.VMEM(flat.shape, F32),
                *tables,
                *[pltpu.VMEM((2, 2, size_x * 2, 128), F32)] * 2,
                *[pltpu.VMEM((2, size_x * 2, 128), F32)] * 4,
                pltpu.VMEM((3, size_x, 512), F32),
                pltpu.VMEM((6, size_x, 512), F32),
                pltpu.SemaphoreType.DMA((5,)),
                *[pltpu.SemaphoreType.DMA((2,))] * 6,
            ],
            compiler_params=pltpu.CompilerParams(
                collective_id=0, has_side_effects=True, vmem_limit_bytes=67043328
            ),
        )(flat, jnp.asarray(qh), jnp.asarray(ql), jnp.asarray(th), jnp.asarray(tl))
        return out.reshape(field.shape)

    placed = (P(("row", "col"), None, None),)
    return jax.shard_map(
        body, mesh=mesh, in_specs=placed, out_specs=P(("row", "col"), None, None), check_vma=False
    )
```

```python
import functools
import math

import jax
import jax.numpy as jnp
import numpy as np
from jax import lax
from jax.experimental import pallas as pl
from jax.experimental.pallas import tpu as pltpu
from jax.sharding import PartitionSpec as P

growth_rate = 0.3
quadratic = 1.0
time_step = 0.2
wave_scale = 4.0
LOGICAL = pl.DeviceIdType.LOGICAL
F32 = jnp.float32
BF16 = jnp.bfloat16


def basis(length):
    n = np.arange(length)
    half = length // 2
    mode = np.where(n <= half, n, n - half)
    angle = 2.0 * np.pi / length * ((mode[:, None] * n[None, :]) % length)
    table = np.where((n <= half)[:, None], np.cos(angle), np.sin(angle))
    scale = np.where((n == 0) | (n == half), 1.0 / length, 2.0 / length)
    return table * np.sqrt(scale)[:, None]


def split(value):
    high = value.astype(BF16)
    return high, (value - high.astype(F32)).astype(BF16)


def dot(left, right):
    return jnp.dot(left, right, preferred_element_type=F32)


def phi_values(argument):
    within = jnp.abs(argument) < 1.0
    inside = jnp.where(within, argument, 0.0)
    outside = jnp.where(within, 2.0, argument)
    series = []
    for degree in (1, 2, 3):
        running = jnp.zeros_like(argument) + 1.0 / math.factorial(11 + degree)
        for exponent in range(10, -1, -1):
            running = running * inside + 1.0 / math.factorial(exponent + degree)
        series.append(running)
    growth_term = jnp.exp(outside)
    closed_one = (growth_term - 1.0) / outside
    closed_two = (growth_term - 1.0 - outside) / (outside * outside)
    closed_three = (growth_term - 1.0 - outside - 0.5 * outside * outside) / (
        outside * outside * outside
    )
    return (
        jnp.where(within, series[0], closed_one),
        jnp.where(within, series[1], closed_two),
        jnp.where(within, series[2], closed_three),
    )


def step_factors(ksq):
    lin = growth_rate - (1.0 - ksq) * (1.0 - ksq)
    scaled = time_step * lin
    half_phi, _, _ = phi_values(0.5 * scaled)
    first_phi, second_phi, third_phi = phi_values(scaled)
    e_half = jnp.exp(0.5 * scaled)
    q_half = 0.5 * time_step * half_phi
    e_full = jnp.exp(scaled)
    f_one = time_step * (first_phi - 3.0 * second_phi + 4.0 * third_phi)
    f_two = time_step * (second_phi - 2.0 * third_phi)
    f_three = time_step * (4.0 * third_phi - second_phi)
    return (e_half, q_half, e_full, f_one, f_two, f_three)


def reaction(values):
    return quadratic * values * values - values * values * values


def wave(index, size):
    mode = jnp.where(index * 2 <= size, index, index - size // 2)
    return wave_scale * mode.astype(F32) / size


def kernel(
    sizes, offsets, field_hbm, qh_hbm, ql_hbm, th_hbm, tl_hbm, out_ref,
    field, qh_ref, ql_ref, th_ref, tl_ref,
    send_p, recv_p, send_f, recv_f, send_i, recv_i, held, factors,
    loaded, psend, precv, fsend, frecv, isend, irecv,
):
    rows, cols, size_x, size_y, size_z = sizes
    devices = rows * cols
    row = lax.axis_index("row")
    col = lax.axis_index("col")
    me = row * cols + col
    quarter = size_y // 4
    count = devices - 1

    z, y = (col // 8) * 2 + row // 4, row % 4
    x, core = (col // 2) % 4, col % 2
    along_zy = {}
    along_xc = {}
    for far in range(4):
        other = (z + far) % 4
        base = (other % 2) * (4 * cols) + (other // 2) * 8
        for near in range(4):
            along_zy[far, near] = base + ((y + near) % 4) * cols
        for near in range(2):
            along_xc[far, near] = ((x + far) % 4) * 2 + (core + near) % 2
    peers = [along_zy[o[0], o[1]] + along_xc[o[2], o[3]] for o in offsets]

    barrier = pltpu.get_barrier_semaphore()
    for other in peers:
        pl.semaphore_signal(barrier, inc=1, device_id=other, device_id_type=LOGICAL)

    loads = [
        pltpu.make_async_copy(source, target, loaded.at[index])
        for index, (source, target) in enumerate(
            ((field_hbm, field), (th_hbm, th_ref), (tl_hbm, tl_ref), (qh_hbm, qh_ref), (ql_hbm, ql_ref))
        )
    ]
    for load in loads:
        load.start()

    def tile(index):
        return pl.ds(pl.multiple_of(index * 4, 4), 4)

    def send(source, target, ssem, rsem):
        for other in peers:
            pltpu.make_async_remote_copy(
                src_ref=source.at[..., tile(other), :],
                dst_ref=target.at[..., tile(me), :],
                send_sem=ssem, recv_sem=rsem,
                device_id=other, device_id_type=LOGICAL,
            ).start()
        target[..., tile(me), :] = source[..., tile(me), :]

    def drain(ref, sem):
        part = ref.at[..., pl.ds(0, count * 4), :]
        pltpu.make_async_copy(part, part, sem).wait()

    def along_zf(values):
        vh, vl = split(values)
        moved = dot(vh, th_ref[...]) + dot(vl, th_ref[...]) + dot(vh, tl_ref[...])
        return split(jnp.concatenate([moved[:size_y], moved[size_y:]], axis=1))

    def along_yf(halves, chunk, target):
        wh, wl = halves
        at = slice(chunk * 2 * quarter, (chunk + 1) * 2 * quarter)
        moved = dot(qh_ref[at, :], wh) + dot(qh_ref[at, :], wl) + dot(ql_ref[at, :], wh)
        for plane in range(2):
            for part in range(2):
                lanes = slice(plane * size_z + part * 128, plane * size_z + part * 128 + 128)
                for k in range(2):
                    start = part * 4 * quarter + plane * 2 + k
                    target[pl.ds(start, quarter, stride=4), :] = moved[
                        k * quarter : (k + 1) * quarter, lanes
                    ]

    def along_yi(source, chunk):
        lines = []
        for k in range(2):
            across = []
            for plane in range(2):
                for part in range(2):
                    start = part * 4 * quarter + plane * 2 + k
                    across.append(source[pl.ds(start, quarter, stride=4), :])
            lines.append(jnp.concatenate(across, axis=1))
        wh, wl = split(jnp.concatenate(lines, axis=0))
        at = slice(chunk * 2 * quarter, (chunk + 1) * 2 * quarter)
        return dot(th_ref[:, at], wh) + dot(th_ref[:, at], wl) + dot(tl_ref[:, at], wh)

    def along_zi(moved):
        vh, vl = split(jnp.concatenate([moved[:, :size_z], moved[:, size_z:]], axis=0))
        return dot(vh, qh_ref[...]) + dot(vl, qh_ref[...]) + dot(vh, ql_ref[...])

    def gathered(source):
        parts = [source[pl.ds(k, size_x, stride=2), :] for k in range(2)]
        gh, gl = split(jnp.concatenate(parts, axis=1))
        return dot(qh_ref[...], gh) + dot(qh_ref[...], gl) + dot(ql_ref[...], gh)

    def scattered(values, target):
        vh, vl = split(values)
        moved = dot(th_ref[...], vh) + dot(th_ref[...], vl) + dot(tl_ref[...], vh)
        for k in range(2):
            target[pl.ds(k, size_x, stride=2), :] = moved[:, k * 128 : k * 128 + 128]

    for load in loads:
        load.wait()
    values = field[...]
    straight = along_zf(values)
    reacted = along_zf(reaction(values))
    for chunk in range(2):
        along_yf(straight, chunk, send_p.at[chunk, 0])
        along_yf(reacted, chunk, send_p.at[chunk, 1])
        if chunk == 0:
            pl.semaphore_wait(barrier, count)
        send(send_p.at[chunk], recv_p.at[chunk], psend.at[chunk], precv.at[chunk])

    part = me // (devices // 2)
    group = me % (devices // 2)
    lane = lax.broadcasted_iota(jnp.int32, (8, 512), 1)
    ky = wave((lane // 128) * quarter + group, size_y)
    kz = wave(part * 128 + lane % 128, size_z)
    kyz = ky * ky + kz * kz

    def factor_rows(block, carry):
        at = pl.ds(pl.multiple_of(block * 8, 8), 8)
        kx = wave(block * 8 + lax.broadcasted_iota(jnp.int32, (8, 512), 0), size_x)
        for index, value in enumerate(step_factors(kx * kx + kyz)):
            factors[index, at, :] = value
        return carry

    lax.fori_loop(0, size_x // 8, factor_rows, 0)

    E_HALF, Q_HALF, E_FULL, F_ONE, F_TWO, F_THREE = range(6)
    for chunk in range(2):
        lanes = slice(chunk * 256, chunk * 256 + 256)
        drain(recv_p.at[chunk], precv.at[chunk])
        state = gathered(recv_p.at[chunk, 0])
        react_u = gathered(recv_p.at[chunk, 1])
        moved = factors[E_HALF, :, lanes] * state
        pushed = factors[Q_HALF, :, lanes] * react_u
        first = moved + pushed
        scattered(first, send_i.at[chunk])
        send(send_i.at[chunk], recv_i.at[chunk], isend.at[chunk], irecv.at[chunk])
        held[0, :, lanes] = moved
        held[1, :, lanes] = factors[E_HALF, :, lanes] * first - pushed
        held[2, :, lanes] = factors[E_FULL, :, lanes] * state + factors[F_ONE, :, lanes] * react_u
    for chunk in range(2):
        drain(send_p.at[chunk], psend.at[chunk])

    for stage in range(4):
        drain(recv_i.at[0], irecv.at[0])
        moved = along_yi(recv_i.at[0], 0)
        drain(recv_i.at[1], irecv.at[1])
        values = along_zi(moved + along_yi(recv_i.at[1], 1))
        for chunk in range(2):
            drain(send_i.at[chunk], isend.at[chunk])
        if stage == 3:
            out_ref[...] = values
            break
        halves = along_zf(reaction(values))
        for chunk in range(2):
            along_yf(halves, chunk, send_f.at[chunk])
            send(send_f.at[chunk], recv_f.at[chunk], fsend.at[chunk], frecv.at[chunk])
        for chunk in range(2):
            lanes = slice(chunk * 256, chunk * 256 + 256)
            drain(recv_f.at[chunk], frecv.at[chunk])
            react = gathered(recv_f.at[chunk])
            if stage == 0:
                spectrum = held[0, :, lanes] + factors[Q_HALF, :, lanes] * react
            if stage == 1:
                spectrum = held[1, :, lanes] + 2.0 * (factors[Q_HALF, :, lanes] * react)
            if stage == 2:
                spectrum = held[2, :, lanes] + factors[F_THREE, :, lanes] * react
            scattered(spectrum, send_i.at[chunk])
            send(send_i.at[chunk], recv_i.at[chunk], isend.at[chunk], irecv.at[chunk])
            if stage < 2:
                held[2, :, lanes] += 2.0 * factors[F_TWO, :, lanes] * react
        for chunk in range(2):
            drain(send_f.at[chunk], fsend.at[chunk])


def hops(offset):
    return sum(min(o, 4 - o) for o in offset[:3])


def schedule():
    every = [(a, b, c, d) for a in range(4) for b in range(4) for c in range(4) for d in range(2)]
    return sorted(every[1:], key=lambda offset: -2 * hops(offset) - offset[3])


def solution(mesh):
    rows, cols = mesh.shape["row"], mesh.shape["col"]
    table = basis(256).astype(np.float32)

    def halves(values):
        high = values.astype(BF16)
        return high, (values - high.astype(np.float32)).astype(BF16)

    qh, ql = halves(table)
    th, tl = halves(np.ascontiguousarray(table.T))

    def body(field):
        planes, size_y, size_z = field.shape
        size_x = planes * rows * cols
        sizes = (rows, cols, size_x, size_y, size_z)
        flat = field.reshape(planes * size_y, size_z)
        hbm = pl.BlockSpec(memory_space=pltpu.HBM)
        tables = [pltpu.VMEM(table.shape, BF16)] * 4
        out = pl.pallas_call(
            functools.partial(kernel, sizes, schedule()),
            out_shape=pltpu.VMEM(flat.shape, F32),
            in_specs=[hbm] * 5,
            out_specs=pl.BlockSpec(memory_space=pltpu.VMEM),
            scratch_shapes=[
                pltpu.VMEM(flat.shape, F32),
                *tables,
                *[pltpu.VMEM((2, 2, size_x * 2, 128), F32)] * 2,
                *[pltpu.VMEM((2, size_x * 2, 128), F32)] * 4,
                pltpu.VMEM((3, size_x, 512), F32),
                pltpu.VMEM((6, size_x, 512), F32),
                pltpu.SemaphoreType.DMA((5,)),
                *[pltpu.SemaphoreType.DMA((2,))] * 6,
            ],
            compiler_params=pltpu.CompilerParams(
                collective_id=0, has_side_effects=True, vmem_limit_bytes=66000000
            ),
        )(flat, jnp.asarray(qh), jnp.asarray(ql), jnp.asarray(th), jnp.asarray(tl))
        return out.reshape(field.shape)

    placed = (P(("row", "col"), None, None),)
    return jax.shard_map(
        body, mesh=mesh, in_specs=placed, out_specs=P(("row", "col"), None, None), check_vma=False
    )
```

```python
import functools
import math

import jax
import jax.numpy as jnp
import numpy as np
from jax import lax
from jax.experimental import pallas as pl
from jax.experimental.pallas import tpu as pltpu
from jax.sharding import PartitionSpec as P

growth_rate = 0.3
quadratic = 1.0
time_step = 0.2
wave_scale = 4.0
LOGICAL = pl.DeviceIdType.LOGICAL
F32 = jnp.float32
BF16 = jnp.bfloat16


def basis(length):
    n = np.arange(length)
    half = length // 2
    mode = np.where(n <= half, n, n - half)
    angle = 2.0 * np.pi / length * ((mode[:, None] * n[None, :]) % length)
    table = np.where((n <= half)[:, None], np.cos(angle), np.sin(angle))
    scale = np.where((n == 0) | (n == half), 1.0 / length, 2.0 / length)
    return table * np.sqrt(scale)[:, None]


def split(value):
    high = value.astype(BF16)
    return high, (value - high.astype(F32)).astype(BF16)


def dot(left, right):
    return jnp.dot(left, right, preferred_element_type=F32)


def phi_values(argument):
    within = jnp.abs(argument) < 1.0
    inside = jnp.where(within, argument, 0.0)
    outside = jnp.where(within, 2.0, argument)
    series = []
    for degree in (1, 2, 3):
        running = jnp.zeros_like(argument) + 1.0 / math.factorial(11 + degree)
        for exponent in range(10, -1, -1):
            running = running * inside + 1.0 / math.factorial(exponent + degree)
        series.append(running)
    growth_term = jnp.exp(outside)
    closed_one = (growth_term - 1.0) / outside
    closed_two = (growth_term - 1.0 - outside) / (outside * outside)
    closed_three = (growth_term - 1.0 - outside - 0.5 * outside * outside) / (
        outside * outside * outside
    )
    return (
        jnp.where(within, series[0], closed_one),
        jnp.where(within, series[1], closed_two),
        jnp.where(within, series[2], closed_three),
    )


def step_factors(ksq):
    lin = growth_rate - (1.0 - ksq) * (1.0 - ksq)
    scaled = time_step * lin
    half_phi, _, _ = phi_values(0.5 * scaled)
    first_phi, second_phi, third_phi = phi_values(scaled)
    e_half = jnp.exp(0.5 * scaled)
    q_half = 0.5 * time_step * half_phi
    e_full = jnp.exp(scaled)
    f_one = time_step * (first_phi - 3.0 * second_phi + 4.0 * third_phi)
    f_two = time_step * (second_phi - 2.0 * third_phi)
    f_three = time_step * (4.0 * third_phi - second_phi)
    return (e_half, q_half, e_full, f_one, f_two, f_three)


def reaction(values):
    return quadratic * values * values - values * values * values


def wave(index, size):
    mode = jnp.where(index * 2 <= size, index, index - size // 2)
    return wave_scale * mode.astype(F32) / size


def kernel(
    sizes, offsets, field_hbm, qh_hbm, ql_hbm, th_hbm, tl_hbm, out_ref,
    field, qh_ref, ql_ref, th_ref, tl_ref,
    send_p, recv_p, send_f, recv_f, send_i, recv_i, held, factors,
    loaded, psend, precv, fsend, frecv, isend, irecv,
):
    rows, cols, size_x, size_y, size_z = sizes
    devices = rows * cols
    row = lax.axis_index("row")
    col = lax.axis_index("col")
    me = row * cols + col
    quarter = size_y // 4
    count = devices - 1

    z, y = (col // 8) * 2 + row // 4, row % 4
    x, core = (col // 2) % 4, col % 2
    along_zy = {}
    along_xc = {}
    for far in range(4):
        other = (z + far) % 4
        base = (other % 2) * (4 * cols) + (other // 2) * 8
        for near in range(4):
            along_zy[far, near] = base + ((y + near) % 4) * cols
        for near in range(2):
            along_xc[far, near] = ((x + far) % 4) * 2 + (core + near) % 2
    peers = [along_zy[o[0], o[1]] + along_xc[o[2], o[3]] for o in offsets]

    barrier = pltpu.get_barrier_semaphore()
    for other in peers:
        pl.semaphore_signal(barrier, inc=1, device_id=other, device_id_type=LOGICAL)

    loads = [
        pltpu.make_async_copy(source, target, loaded.at[index])
        for index, (source, target) in enumerate(
            ((field_hbm, field), (th_hbm, th_ref), (tl_hbm, tl_ref), (qh_hbm, qh_ref), (ql_hbm, ql_ref))
        )
    ]
    for load in loads:
        load.start()

    def tile(index):
        return pl.ds(pl.multiple_of(index * 4, 4), 4)

    def send(source, target, ssem, rsem):
        for other in peers:
            pltpu.make_async_remote_copy(
                src_ref=source.at[..., tile(other), :],
                dst_ref=target.at[..., tile(me), :],
                send_sem=ssem, recv_sem=rsem,
                device_id=other, device_id_type=LOGICAL,
            ).start()
        target[..., tile(me), :] = source[..., tile(me), :]

    def drain(ref, sem):
        part = ref.at[..., pl.ds(0, count * 4), :]
        pltpu.make_async_copy(part, part, sem).wait()

    def along_zf(values):
        vh, vl = split(values)
        moved = dot(vh, th_ref[...]) + dot(vl, th_ref[...]) + dot(vh, tl_ref[...])
        return split(jnp.concatenate([moved[:size_y], moved[size_y:]], axis=1))

    def along_yf(halves, chunk, target):
        wh, wl = halves
        at = slice(chunk * 2 * quarter, (chunk + 1) * 2 * quarter)
        moved = dot(qh_ref[at, :], wh) + dot(qh_ref[at, :], wl) + dot(ql_ref[at, :], wh)
        for plane in range(2):
            for part in range(2):
                lanes = slice(plane * size_z + part * 128, plane * size_z + part * 128 + 128)
                for k in range(2):
                    start = part * 4 * quarter + plane * 2 + k
                    target[pl.ds(start, quarter, stride=4), :] = moved[
                        k * quarter : (k + 1) * quarter, lanes
                    ]

    def along_yi(source, chunk):
        lines = []
        for k in range(2):
            across = []
            for plane in range(2):
                for part in range(2):
                    start = part * 4 * quarter + plane * 2 + k
                    across.append(source[pl.ds(start, quarter, stride=4), :])
            lines.append(jnp.concatenate(across, axis=1))
        wh, wl = split(jnp.concatenate(lines, axis=0))
        at = slice(chunk * 2 * quarter, (chunk + 1) * 2 * quarter)
        return dot(th_ref[:, at], wh) + dot(th_ref[:, at], wl) + dot(tl_ref[:, at], wh)

    def along_zi(moved):
        vh, vl = split(jnp.concatenate([moved[:, :size_z], moved[:, size_z:]], axis=0))
        return dot(vh, qh_ref[...]) + dot(vl, qh_ref[...]) + dot(vh, ql_ref[...])

    def gathered(source):
        parts = [source[pl.ds(k, size_x, stride=2), :] for k in range(2)]
        gh, gl = split(jnp.concatenate(parts, axis=1))
        return dot(qh_ref[...], gh) + dot(qh_ref[...], gl) + dot(ql_ref[...], gh)

    def scattered(values, target):
        vh, vl = split(values)
        moved = dot(th_ref[...], vh) + dot(th_ref[...], vl) + dot(tl_ref[...], vh)
        for k in range(2):
            target[pl.ds(k, size_x, stride=2), :] = moved[:, k * 128 : k * 128 + 128]

    for load in loads:
        load.wait()
    values = field[...]
    straight = along_zf(values)
    reacted = along_zf(reaction(values))
    for chunk in range(2):
        along_yf(straight, chunk, send_p.at[chunk, 0])
        along_yf(reacted, chunk, send_p.at[chunk, 1])
        if chunk == 0:
            pl.semaphore_wait(barrier, count)
        send(send_p.at[chunk], recv_p.at[chunk], psend.at[chunk], precv.at[chunk])

    part = me // (devices // 2)
    group = me % (devices // 2)
    lane = lax.broadcasted_iota(jnp.int32, (8, 512), 1)
    ky = wave((lane // 128) * quarter + group, size_y)
    kz = wave(part * 128 + lane % 128, size_z)
    kyz = ky * ky + kz * kz

    def factor_rows(block, carry):
        at = pl.ds(pl.multiple_of(block * 8, 8), 8)
        kx = wave(block * 8 + lax.broadcasted_iota(jnp.int32, (8, 512), 0), size_x)
        for index, value in enumerate(step_factors(kx * kx + kyz)):
            factors[index, at, :] = value
        return carry

    lax.fori_loop(0, size_x // 8, factor_rows, 0)

    E_HALF, Q_HALF, E_FULL, F_ONE, F_TWO, F_THREE = range(6)
    for chunk in range(2):
        lanes = slice(chunk * 256, chunk * 256 + 256)
        drain(recv_p.at[chunk], precv.at[chunk])
        state = gathered(recv_p.at[chunk, 0])
        react_u = gathered(recv_p.at[chunk, 1])
        moved = factors[E_HALF, :, lanes] * state
        pushed = factors[Q_HALF, :, lanes] * react_u
        first = moved + pushed
        scattered(first, send_i.at[chunk])
        send(send_i.at[chunk], recv_i.at[chunk], isend.at[chunk], irecv.at[chunk])
        held[0, :, lanes] = moved
        held[1, :, lanes] = factors[E_HALF, :, lanes] * first - pushed
        held[2, :, lanes] = factors[E_FULL, :, lanes] * state + factors[F_ONE, :, lanes] * react_u
    for chunk in range(2):
        drain(send_p.at[chunk], psend.at[chunk])

    for stage in range(4):
        drain(recv_i.at[0], irecv.at[0])
        moved = along_yi(recv_i.at[0], 0)
        drain(recv_i.at[1], irecv.at[1])
        values = along_zi(moved + along_yi(recv_i.at[1], 1))
        for chunk in range(2):
            drain(send_i.at[chunk], isend.at[chunk])
        if stage == 3:
            out_ref[...] = values
            break
        halves = along_zf(reaction(values))
        for chunk in range(2):
            along_yf(halves, chunk, send_f.at[chunk])
            send(send_f.at[chunk], recv_f.at[chunk], fsend.at[chunk], frecv.at[chunk])
        for chunk in range(2):
            lanes = slice(chunk * 256, chunk * 256 + 256)
            drain(recv_f.at[chunk], frecv.at[chunk])
            react = gathered(recv_f.at[chunk])
            if stage == 0:
                spectrum = held[0, :, lanes] + factors[Q_HALF, :, lanes] * react
            if stage == 1:
                spectrum = held[1, :, lanes] + 2.0 * (factors[Q_HALF, :, lanes] * react)
            if stage == 2:
                spectrum = held[2, :, lanes] + factors[F_THREE, :, lanes] * react
            scattered(spectrum, send_i.at[chunk])
            send(send_i.at[chunk], recv_i.at[chunk], isend.at[chunk], irecv.at[chunk])
            if stage < 2:
                held[2, :, lanes] += 2.0 * factors[F_TWO, :, lanes] * react
        for chunk in range(2):
            drain(send_f.at[chunk], fsend.at[chunk])


def hops(offset):
    return sum(min(o, 4 - o) for o in offset[:3])


def schedule():
    every = [(a, b, c, d) for a in range(4) for b in range(4) for c in range(4) for d in range(2)]
    return sorted(every[1:], key=lambda offset: -2 * hops(offset) - offset[3])


def solution(mesh):
    rows, cols = mesh.shape["row"], mesh.shape["col"]
    table = basis(256).astype(np.float32)

    def halves(values):
        high = values.astype(BF16)
        return high, (values - high.astype(np.float32)).astype(BF16)

    qh, ql = halves(table)
    th, tl = halves(np.ascontiguousarray(table.T))

    def body(field):
        planes, size_y, size_z = field.shape
        size_x = planes * rows * cols
        sizes = (rows, cols, size_x, size_y, size_z)
        flat = field.reshape(planes * size_y, size_z)
        hbm = pl.BlockSpec(memory_space=pltpu.HBM)
        tables = [pltpu.VMEM(table.shape, BF16)] * 4
        out = pl.pallas_call(
            functools.partial(kernel, sizes, schedule()),
            out_shape=pltpu.VMEM(flat.shape, F32),
            in_specs=[hbm] * 5,
            out_specs=pl.BlockSpec(memory_space=pltpu.VMEM),
            scratch_shapes=[
                pltpu.VMEM(flat.shape, F32),
                *tables,
                *[pltpu.VMEM((2, 2, size_x * 2 + 8, 128), F32)] * 2,
                *[pltpu.VMEM((2, size_x * 2 + 8, 128), F32)] * 4,
                pltpu.VMEM((3, size_x, 512), F32),
                pltpu.VMEM((6, size_x, 512), F32),
                pltpu.SemaphoreType.DMA((5,)),
                *[pltpu.SemaphoreType.DMA((2,))] * 6,
            ],
            compiler_params=pltpu.CompilerParams(
                collective_id=0, has_side_effects=True, vmem_limit_bytes=66000000
            ),
        )(flat, jnp.asarray(qh), jnp.asarray(ql), jnp.asarray(th), jnp.asarray(tl))
        return out.reshape(field.shape)

    placed = (P(("row", "col"), None, None),)
    return jax.shard_map(
        body, mesh=mesh, in_specs=placed, out_specs=P(("row", "col"), None, None), check_vma=False
    )
```

```python
import functools
import math

import jax
import jax.numpy as jnp
import numpy as np
from jax import lax
from jax.experimental import pallas as pl
from jax.experimental.pallas import tpu as pltpu
from jax.sharding import PartitionSpec as P

growth_rate = 0.3
quadratic = 1.0
time_step = 0.2
wave_scale = 4.0
LOGICAL = pl.DeviceIdType.LOGICAL
F32 = jnp.float32
BF16 = jnp.bfloat16


def basis(length):
    n = np.arange(length)
    half = length // 2
    mode = np.where(n <= half, n, n - half)
    angle = 2.0 * np.pi / length * ((mode[:, None] * n[None, :]) % length)
    table = np.where((n <= half)[:, None], np.cos(angle), np.sin(angle))
    scale = np.where((n == 0) | (n == half), 1.0 / length, 2.0 / length)
    return table * np.sqrt(scale)[:, None]


def split(value):
    high = value.astype(BF16)
    return high, (value - high.astype(F32)).astype(BF16)


def dot(left, right):
    return jnp.dot(left, right, preferred_element_type=F32)


def phi_values(argument):
    within = jnp.abs(argument) < 1.0
    inside = jnp.where(within, argument, 0.0)
    outside = jnp.where(within, 2.0, argument)
    series = []
    for degree in (1, 2, 3):
        running = jnp.zeros_like(argument) + 1.0 / math.factorial(11 + degree)
        for exponent in range(10, -1, -1):
            running = running * inside + 1.0 / math.factorial(exponent + degree)
        series.append(running)
    growth_term = jnp.exp(outside)
    closed_one = (growth_term - 1.0) / outside
    closed_two = (growth_term - 1.0 - outside) / (outside * outside)
    closed_three = (growth_term - 1.0 - outside - 0.5 * outside * outside) / (
        outside * outside * outside
    )
    return (
        jnp.where(within, series[0], closed_one),
        jnp.where(within, series[1], closed_two),
        jnp.where(within, series[2], closed_three),
    )


def step_factors(ksq):
    lin = growth_rate - (1.0 - ksq) * (1.0 - ksq)
    scaled = time_step * lin
    half_phi, _, _ = phi_values(0.5 * scaled)
    first_phi, second_phi, third_phi = phi_values(scaled)
    e_half = jnp.exp(0.5 * scaled)
    q_half = 0.5 * time_step * half_phi
    e_full = jnp.exp(scaled)
    f_one = time_step * (first_phi - 3.0 * second_phi + 4.0 * third_phi)
    f_two = time_step * (second_phi - 2.0 * third_phi)
    f_three = time_step * (4.0 * third_phi - second_phi)
    return (e_half, q_half, e_full, f_one, f_two, f_three)


def reaction(values):
    return quadratic * values * values - values * values * values


def wave(index, size):
    mode = jnp.where(index * 2 <= size, index, index - size // 2)
    return wave_scale * mode.astype(F32) / size


def kernel(
    sizes, offsets, field_hbm, tables_hbm, out_ref, field, tables,
    send_p0, recv_p0, send_p1, recv_p1, send_f0, recv_f0, send_f1, recv_f1,
    send_i0, recv_i0, send_i1, recv_i1, held, gains,
    loaded, psend, precv, fsend, frecv, isend, irecv,
):
    rows, cols, size_x, size_y, size_z = sizes
    devices = rows * cols
    row = lax.axis_index("row")
    col = lax.axis_index("col")
    me = row * cols + col
    quarter = size_y // 4
    count = devices - 1

    z, y = (col // 8) * 2 + row // 4, row % 4
    x, core = (col // 2) % 4, col % 2
    along_zy = {}
    along_xc = {}
    for far in range(4):
        other = (z + far) % 4
        base = (other % 2) * (4 * cols) + (other // 2) * 8
        for near in range(4):
            along_zy[far, near] = base + ((y + near) % 4) * cols
        for near in range(2):
            along_xc[far, near] = ((x + far) % 4) * 2 + (core + near) % 2
    peers = [along_zy[o[0], o[1]] + along_xc[o[2], o[3]] for o in offsets]

    barrier = pltpu.get_barrier_semaphore()
    for other in peers:
        pl.semaphore_signal(barrier, inc=1, device_id=other, device_id_type=LOGICAL)

    loads = [
        pltpu.make_async_copy(field_hbm, field, loaded.at[0]),
        pltpu.make_async_copy(tables_hbm, tables, loaded.at[1]),
    ]
    qh_ref, ql_ref, th_ref, tl_ref, xqh_ref, xql_ref, xth_ref, xtl_ref = (
        tables.at[index] for index in range(8)
    )
    for load in loads:
        load.start()

    def send(source, target, ssem, rsem):
        depth = source.shape[0] // devices

        def tile(index):
            return pl.ds(pl.multiple_of(index * depth, depth), depth)

        for other in peers:
            pltpu.make_async_remote_copy(
                src_ref=source.at[tile(other), :],
                dst_ref=target.at[tile(me), :],
                send_sem=ssem, recv_sem=rsem,
                device_id=other, device_id_type=LOGICAL,
            ).start()
        target[tile(me), :] = source[tile(me), :]

    def drain(ref, sem):
        part = ref.at[pl.ds(0, count * (ref.shape[0] // devices)), :]
        pltpu.make_async_copy(part, part, sem).wait()

    def first_rows(whole, cut, entry):
        def at(plane, chunk, k):
            if plane == 0:
                return whole, 8, entry * 4 + chunk * 2 + k
            return cut.at[chunk], 4, entry * 2 + k

        return at

    def forward_rows(whole, cut):
        def at(plane, chunk, k):
            return (cut.at[chunk], 2, k) if plane else (whole, 4, chunk * 2 + k)

        return at

    def inverse_rows(whole, cut):
        def at(plane, chunk, k):
            return (whole, 4, chunk * 2 + k) if plane else (cut.at[chunk], 2, k)

        return at

    def lines_of(place, start, length):
        ref, depth, row_in = place
        return ref, pl.ds(start * depth + row_in, length, stride=depth)

    def read(place, start, length):
        ref, at = lines_of(place, start, length)
        return ref[at, :]

    def write(place, start, length, values):
        ref, at = lines_of(place, start, length)
        ref[at, :] = values

    def send_first(index):
        if index == 0:
            send(send_p0, recv_p0, psend.at[0], precv.at[0])
        else:
            send(send_p1.at[index - 1], recv_p1.at[index - 1], psend.at[index], precv.at[index])

    def send_forward(index):
        if index == 0:
            send(send_f0, recv_f0, fsend.at[0], frecv.at[0])
        else:
            send(send_f1.at[index - 1], recv_f1.at[index - 1], fsend.at[index], frecv.at[index])

    def send_inverse(index):
        if index == 2:
            send(send_i0, recv_i0, isend.at[2], irecv.at[2])
        else:
            send(send_i1.at[index], recv_i1.at[index], isend.at[index], irecv.at[index])

    def finish_first(index, whole, cut, sem):
        drain(whole if index == 0 else cut.at[index - 1], sem.at[index])

    def finish_inverse(index, whole, cut, sem):
        drain(whole if index == 2 else cut.at[index], sem.at[index])

    def along_zf(values):
        vh, vl = split(values)
        return split(dot(vh, th_ref[...]) + dot(vl, th_ref[...]) + dot(vh, tl_ref[...]))

    def along_yf(halves, plane, chunk, place):
        wh, wl = halves
        at = slice(chunk * 2 * quarter, (chunk + 1) * 2 * quarter)
        moved = dot(qh_ref[at, :], wh) + dot(qh_ref[at, :], wl) + dot(ql_ref[at, :], wh)
        for part in range(2):
            for k in range(2):
                lanes = slice(part * 128, part * 128 + 128)
                values = moved[k * quarter : (k + 1) * quarter, lanes]
                write(place(plane, chunk, k), part * quarter, quarter, values)

    def physical(plane):
        lines = []
        place = inverse_rows(recv_i0, recv_i1)
        for chunk in range(2):
            for k in range(2):
                across = [read(place(plane, chunk, k), part * quarter, quarter) for part in range(2)]
                lines.append(jnp.concatenate(across, axis=1))
        wh, wl = split(jnp.concatenate(lines, axis=0))
        moved = dot(th_ref[...], wh) + dot(th_ref[...], wl) + dot(tl_ref[...], wh)
        vh, vl = split(moved)
        return dot(vh, qh_ref[...]) + dot(vl, qh_ref[...]) + dot(vh, ql_ref[...])

    def gathered(place, chunk):
        lines = []
        for plane in range(2):
            across = [read(place(plane, chunk, k), 0, size_x // 2) for k in range(2)]
            lines.append(jnp.concatenate(across, axis=1))
        gh, gl = split(jnp.concatenate(lines, axis=0))
        return dot(xqh_ref[...], gh) + dot(xqh_ref[...], gl) + dot(xql_ref[...], gh)

    def scattered(values, chunk):
        vh, vl = split(values)
        moved = dot(xth_ref[...], vh) + dot(xth_ref[...], vl) + dot(xtl_ref[...], vh)
        for plane in range(2):
            rows_x = slice(plane * (size_x // 2), (plane + 1) * (size_x // 2))
            for k in range(2):
                place = inverse_rows(send_i0, send_i1)(plane, chunk, k)
                write(place, 0, size_x // 2, moved[rows_x, k * 128 : k * 128 + 128])

    for load in loads:
        load.wait()
    for plane in range(2):
        values = field[plane * size_y : (plane + 1) * size_y, :]
        straight = along_zf(values)
        reacted = along_zf(reaction(values))
        for chunk in range(2):
            at = plane * 2 + chunk
            along_yf(straight, plane, chunk, first_rows(send_p0, send_p1, 0))
            along_yf(reacted, plane, chunk, first_rows(send_p0, send_p1, 1))
            if at == 1:
                pl.semaphore_wait(barrier, count)
            if at > 0:
                send_first(at - 1)

    part = me // (devices // 2)
    group = me % (devices // 2)
    lane = lax.broadcasted_iota(jnp.int32, (8, 512), 1)
    ky = wave((lane // 128) * quarter + group, size_y)
    kz = wave(part * 128 + lane % 128, size_z)
    kyz = ky * ky + kz * kz

    def factor_rows(block, carry):
        at = pl.ds(pl.multiple_of(block * 8, 8), 8)
        kx = wave(block * 8 + lax.broadcasted_iota(jnp.int32, (8, 512), 0), size_x)
        e_half, q_half, e_full, f_one, f_two, f_three = step_factors(kx * kx + kyz)
        gains[0, at, :] = q_half
        gains[1, at, :] = 2.0 * q_half
        gains[2, at, :] = f_three
        gains[3, at, :] = 2.0 * f_two
        gains[4, at, :] = e_half
        gains[5, at, :] = e_full
        gains[6, at, :] = f_one
        return carry

    lax.fori_loop(0, size_x // 8, factor_rows, 0)

    finish_first(0, recv_p0, recv_p1, precv)
    known = []
    for chunk in range(2):
        lanes = slice(chunk * 256, chunk * 256 + 256)
        finish_first(1 + chunk, recv_p0, recv_p1, precv)
        state = gathered(first_rows(recv_p0, recv_p1, 0), chunk)
        react_u = gathered(first_rows(recv_p0, recv_p1, 1), chunk)
        moved = gains[4, :, lanes] * state
        pushed = gains[0, :, lanes] * react_u
        scattered(moved + pushed, chunk)
        send_inverse(chunk)
        known.append((lanes, state, react_u, moved, pushed))
    send_inverse(2)
    for lanes, state, react_u, moved, pushed in known:
        held[0, :, lanes] = moved
        held[1, :, lanes] = gains[4, :, lanes] * (moved + pushed) - pushed
        held[2, :, lanes] = gains[5, :, lanes] * state + gains[6, :, lanes] * react_u
    for index in range(3):
        finish_first(index, send_p0, send_p1, psend)

    def arrived(plane):
        for index in (0, 1) if plane == 0 else (2,):
            finish_inverse(index, recv_i0, recv_i1, irecv)

    def stage(index, carry):
        for plane in range(2):
            arrived(plane)
            halves = along_zf(reaction(physical(plane)))
            for chunk in range(2):
                at = plane * 2 + chunk
                along_yf(halves, plane, chunk, forward_rows(send_f0, send_f1))
                if at > 0:
                    send_forward(at - 1)
        for part in range(3):
            finish_inverse(part, send_i0, send_i1, isend)
        finish_first(0, recv_f0, recv_f1, frecv)
        known = []
        for chunk in range(2):
            lanes = slice(chunk * 256, chunk * 256 + 256)
            finish_first(1 + chunk, recv_f0, recv_f1, frecv)
            react = gathered(forward_rows(recv_f0, recv_f1), chunk)
            scattered(held[index, :, lanes] + gains[index, :, lanes] * react, chunk)
            send_inverse(chunk)
            known.append((lanes, react))
        send_inverse(2)
        for lanes, react in known:
            held[2, :, lanes] += gains[3, :, lanes] * react
        for part in range(3):
            finish_first(part, send_f0, send_f1, fsend)
        return carry

    lax.fori_loop(0, 3, stage, 0)
    for plane in range(2):
        arrived(plane)
        out_ref[plane * size_y : (plane + 1) * size_y, :] = physical(plane)
    for part in range(3):
        finish_inverse(part, send_i0, send_i1, isend)


def hops(offset):
    return sum(min(o, 4 - o) for o in offset[:3])


def schedule():
    every = [(a, b, c, d) for a in range(4) for b in range(4) for c in range(4) for d in range(2)]
    return sorted(every[1:], key=lambda offset: -2 * hops(offset) - offset[3])


def solution(mesh):
    rows, cols = mesh.shape["row"], mesh.shape["col"]
    table = basis(256).astype(np.float32)

    def halves(values):
        high = values.astype(BF16)
        return high, (values - high.astype(np.float32)).astype(BF16)

    along_x = np.concatenate([table[:, 0::2], table[:, 1::2]], axis=1)
    tables = np.stack([h for t in (table, table.T, along_x, along_x.T) for h in halves(t)])

    def body(field):
        planes, size_y, size_z = field.shape
        size_x = planes * rows * cols
        sizes = (rows, cols, size_x, size_y, size_z)
        flat = field.reshape(planes * size_y, size_z)
        hbm = pl.BlockSpec(memory_space=pltpu.HBM)
        out = pl.pallas_call(
            functools.partial(kernel, sizes, schedule()),
            out_shape=pltpu.VMEM(flat.shape, F32),
            in_specs=[hbm] * 2,
            out_specs=pl.BlockSpec(memory_space=pltpu.VMEM),
            scratch_shapes=[
                pltpu.VMEM(flat.shape, F32),
                pltpu.VMEM(tables.shape, BF16),
                *[pltpu.VMEM((size_x * 4 + 8, 128), F32)] * 2,
                *[pltpu.VMEM((2, size_x * 2 + 8, 128), F32)] * 2,
                *[pltpu.VMEM((size_x * 2 + 8, 128), F32)] * 2,
                *[pltpu.VMEM((2, size_x + 8, 128), F32)] * 2,
                *[pltpu.VMEM((size_x * 2 + 8, 128), F32)] * 2,
                *[pltpu.VMEM((2, size_x + 8, 128), F32)] * 2,
                pltpu.VMEM((3, size_x, 512), F32),
                pltpu.VMEM((7, size_x, 512), F32),
                pltpu.SemaphoreType.DMA((2,)),
                *[pltpu.SemaphoreType.DMA((3,))] * 6,
            ],
            compiler_params=pltpu.CompilerParams(
                collective_id=0, has_side_effects=True, vmem_limit_bytes=66000000
            ),
        )(flat, jnp.asarray(tables))
        return out.reshape(field.shape)

    placed = (P(("row", "col"), None, None),)
    return jax.shard_map(
        body, mesh=mesh, in_specs=placed, out_specs=P(("row", "col"), None, None), check_vma=False
    )
```
